32 devices in a mesh: gx: 8 (over y, x, core), gy: 4 (over z).
Axes of the slice: x: 2, y: 2, z: 4, core: 2. Of those that a mesh axis runs over, the one named last changes fastest.
Arguments:
- queries: bfloat16 [512, 2048], P(('gx', 'gy')), may hold values from -6 to 6
- probe_dev: int32 [512, 16], P(('gx', 'gy')), may hold values from 0 to 31, all different within a row; in each aligned block of 16 rows (0 to 15, 16 to 31, ...) at most 10 rows name the same one
- probe_list: int32 [512, 16], P(('gx', 'gy')), may hold values from 0 to 15
- documents: bfloat16 [512, 256, 2048], P(('gx', 'gy')), may hold values from -6 to 6
- lengths: int32 [512], P(('gx', 'gy')), may hold values from 96 to 256, as said below
- short_dev: int32 [512, 32], P(('gx', 'gy')), may hold values from 0 to 31, all different within a row; in each aligned block of 16 rows (0 to 15, 16 to 31, ...) at most 16 rows name the same one
- short_list: int32 [512, 32], P(('gx', 'gy')), may hold values from 0 to 15
- short_row: int32 [512, 32], P(('gx', 'gy')), may hold values from 0 to 95
Outputs:
- prefix_top: float32 [512, 32], P(('gx', 'gy'))
- rescored: float32 [512, 32], P(('gx', 'gy'))
The draws below stay inside these ranges and needn't reach their ends.
Inputs may be any that keep to these rules, and one draw needn't show every extreme that they name: `lengths`: every list holds at least 96 documents, and in every draw some list is full. `probe_dev`: the 16 entries of a query name different devices. Among the 16 queries of one device, no device is named more than 10 times, and some device is named exactly 10 times. `short_dev`: the 32 entries of a query name different devices. Among the 16 queries of one device, no device is named more than 16 times, and some device is named exactly 16 times.
All inputs are finite; a program needn't handle non-finite values.
Results may differ from the reference program's by a relative error of at most 0.0029.
Values may be sent and summed in bfloat16 or wider, within the bound.
A program may use at most 128 MiB of HBM per device.

```python
import math
import jax
import jax.numpy as jnp
import numpy as np
from jax import lax

QRY_DEV = 16
LISTS_DEV = 16
ROWS = 256
LEN_MIN = 96
PREFIX = 256
FULL = 2048
PROBES = 16
TOPK = 32
SHORT = 32
QUERIES = 512
LISTS = 512
CAP = 16
PCAP = 10
DEVICES = 32


def draw_lengths(key, part):
    first_key, second_key = jax.random.split(jax.random.fold_in(key, 17))
    counts = jax.random.randint(first_key, (LISTS,), LEN_MIN, ROWS + 1)
    full_spot = jax.random.randint(second_key, (), 0, LISTS)
    return jnp.where(jnp.arange(LISTS) == full_spot, ROWS, counts).astype(jnp.int32)


def plant(entries, key, smallest, top_value):
    spot = [jax.random.randint(jax.random.fold_in(key, axis), (), 0, length) for axis, length in enumerate(entries.shape)]
    main_axis = entries.shape.index(max(entries.shape))
    neighbour = spot[:main_axis] + [(spot[main_axis] + 1) % entries.shape[main_axis]] + spot[main_axis + 1:]
    return entries.at[tuple(spot)].set(smallest).at[tuple(neighbour)].set(top_value)


def steps_of(rng, extent, cuts, least, largest):
    factor_of, own = 1.0, jax.random.fold_in(rng, 6)
    for position, blocks in cuts:
        steps = jnp.exp(jax.random.uniform(jax.random.fold_in(own, position), (blocks,), jnp.float32, least / len(cuts), largest / len(cuts)))
        factor_of = factor_of * jnp.repeat(steps, extent[position] // blocks).reshape([-1 if axis == position else 1 for axis in range(len(extent))])
    return factor_of


def deal_out(own_key, own, number, rows, number_of, top, reach, skew):
    ranking = jax.random.permutation(own_key, number_of)
    heavy_load, ordinary = load_shares(number_of, rows * top, reach, skew, True), load_shares(number_of, rows * top, reach, skew, False)
    places = jnp.arange(number_of)

    def named(sizes, offset_by):
        used = int((sizes > 0).sum())
        fixed = max(1, used // 4)
        shifted = fixed + (places - fixed + offset_by * (used - fixed)) % max(1, number_of - fixed)
        return jnp.zeros((number_of,), jnp.int32).at[ranking[jnp.where(places < fixed, places, shifted)]].set(jnp.asarray(sizes, jnp.int32))

    sizes = jnp.where(number % 4 == 0, named(heavy_load, number // 4), named(ordinary, number - number // 4 - 1))
    mixed = jax.random.permutation(jax.random.fold_in(own, 3), number_of)
    giver, taker = mixed[0:number_of // 2 * 2:2], mixed[1:number_of // 2 * 2:2]
    margin = jnp.minimum(sizes[giver] - 1, reach - sizes[taker]) // 2
    margin = jnp.where((giver == ranking[0]) | (taker == ranking[0]) | (sizes[taker] == 0), 0, jnp.maximum(margin, 0))
    shifted = jax.random.randint(jax.random.fold_in(own, 4), (number_of // 2,), 0, 1 << 20) % (margin + 1)
    sizes = sizes.at[giver].add(-shifted).at[taker].add(shifted)
    members = jnp.searchsorted(jnp.cumsum(sizes), jnp.arange(rows * top), side="right").astype(jnp.int32)
    table = members.reshape(top, rows).T
    table = table[jax.random.permutation(jax.random.fold_in(own, 1), rows)]
    offset_by = jax.random.randint(jax.random.fold_in(own, 2), (rows, 1), 0, top)
    return jnp.take_along_axis(table, (jnp.arange(top)[None, :] + offset_by) % top, axis=1)


def load_shares(count, total, reach, skew, full):
    portions = [(1 << 20) // math.isqrt(grade ** skew) + 1 for grade in range(1, count + 1)]
    largest = reach if full else min(reach, max(-(-total // count), total * portions[0] // sum(portions)))
    least = 1 if total - largest >= count - 1 else 0
    given, rest = [largest] + [least] * (count - 1), total - largest - least * (count - 1)
    while rest > 0:
        movable = [i for i in range(1, count) if given[i] < largest] or [i for i in range(1, count) if given[i] < reach]
        whole, budget = sum([portions[i] for i in movable]), rest
        for i in movable:
            extra = min(reach - given[i], max(1, budget * portions[i] // whole), rest)
            given[i] = given[i] + extra
            rest = rest - extra
    return np.array(given)


def gaussian(rng, shape, deviation, bound, cuts=(), held_as=jnp.bfloat16):
    result = jax.random.normal(rng, shape, jnp.float32) * deviation
    if len(cuts) > 0:
        result = steps_of(rng, shape, cuts, -0.22, 0.18) * result
    return jnp.clip(result, min=-bound, max=bound).astype(held_as)


def setup_inputs(seed: int = 0) -> dict:
    key_of = jax.random.split(jax.random.key(seed), 9)
    queries = gaussian(key_of[0], (QUERIES, FULL), 1.0, 6.0, ((0, 32),))
    probe_dev_keys = jax.random.split(jax.random.fold_in(key_of[1], 1), QUERIES // QRY_DEV)
    probe_dev_turns = jax.random.permutation(jax.random.fold_in(key_of[1], 3), QUERIES // QRY_DEV)
    probe_dev = jax.vmap(lambda own, number: deal_out(jax.random.fold_in(key_of[1], 2), own, number, QRY_DEV, DEVICES, PROBES, PCAP, 2))(probe_dev_keys, probe_dev_turns).reshape((QUERIES, PROBES))
    probe_list = plant(jax.random.randint(key_of[2], (QUERIES, PROBES), 0, LISTS_DEV), jax.random.fold_in(key_of[2], 1), 0, LISTS_DEV - 1).astype(jnp.int32)
    documents = gaussian(key_of[3], (LISTS, ROWS, FULL), 1.0, 6.0, ((0, 32),))
    lengths = draw_lengths(jax.random.fold_in(key_of[8], 71), 0)
    short_dev_keys = jax.random.split(jax.random.fold_in(key_of[5], 1), QUERIES // QRY_DEV)
    short_dev_turns = jax.random.permutation(jax.random.fold_in(key_of[5], 3), QUERIES // QRY_DEV)
    short_dev = jax.vmap(lambda own, number: deal_out(jax.random.fold_in(key_of[5], 2), own, number, QRY_DEV, DEVICES, SHORT, CAP, 1))(short_dev_keys, short_dev_turns).reshape((QUERIES, SHORT))
    short_list = plant(jax.random.randint(key_of[6], (QUERIES, SHORT), 0, LISTS_DEV), jax.random.fold_in(key_of[6], 1), 0, LISTS_DEV - 1).astype(jnp.int32)
    short_row = plant(jax.random.randint(key_of[7], (QUERIES, SHORT), 0, LEN_MIN), jax.random.fold_in(key_of[7], 1), 0, LEN_MIN - 1).astype(jnp.int32)
    return dict(queries=queries, probe_dev=probe_dev, probe_list=probe_list, documents=documents, lengths=lengths, short_dev=short_dev, short_list=short_list, short_row=short_row)


def unit_rows(values):
    return values / jnp.sqrt(1.0 + lax.optimization_barrier(jnp.sum(values * values, axis=1, keepdims=True)))

def top_values(values, count):
    return -jnp.sort(-values, axis=-1)[..., :count]

def reference(queries, probe_dev, probe_list, documents, lengths, short_dev, short_list, short_row):
    query_float = queries.astype(jnp.float32)
    prefix_unit = unit_rows(query_float[:, :PREFIX]).astype(jnp.bfloat16)
    full_unit = unit_rows(query_float).astype(jnp.bfloat16)
    doc_prefix = documents[:, :, :PREFIX]
    probes = (probe_dev * LISTS_DEV + probe_list).astype(jnp.int32)
    query_total = queries.shape[0]
    block_rows = 64 if query_total % 64 == 0 else query_total

    def top_block(inputs):
        prefix_block, probe_block = inputs
        gathered = doc_prefix[probe_block]
        scores = jnp.einsum('bd,bprd->bpr', prefix_block.astype(jnp.float32), gathered.astype(jnp.float32))
        valid_rows = jnp.arange(ROWS)[None, None, :] < lengths[probe_block][:, :, None]
        masked = jnp.where(valid_rows, scores, -jnp.inf).reshape(prefix_block.shape[0], -1)
        return top_values(masked, TOPK)
    prefix_top = lax.map(top_block, (prefix_unit.reshape(-1, block_rows, PREFIX), probes.reshape(-1, block_rows, PROBES))).reshape(query_total, TOPK)

    def rescore_block(inputs):
        unit_block, dev_block, list_block, row_block = inputs
        list_index = (dev_block * LISTS_DEV + list_block).astype(jnp.int32)
        vectors = documents[list_index, row_block.astype(jnp.int32)]
        return jnp.einsum('bsf,bf->bs', vectors.astype(jnp.float32), unit_block.astype(jnp.float32))
    rescored = lax.map(rescore_block, (full_unit.reshape(-1, block_rows, FULL), short_dev.reshape(-1, block_rows, SHORT), short_list.reshape(-1, block_rows, SHORT), short_row.reshape(-1, block_rows, SHORT))).reshape(query_total, SHORT)
    return (prefix_top, rescored)
```

```python
import functools

import jax
import jax.numpy as jnp
from jax import lax
from jax.experimental import pallas as pl
from jax.experimental.pallas import tpu as pltpu
from jax.sharding import PartitionSpec as P

PREFIX = 256
TOPK = 32
SHORT_ROWS = 96
AXES = ("gx", "gy")
LANES = 128
TILE = 256
WIDTH = 256
NT = (((1,), (1,)), ((), ()))
MESH = pl.DeviceIdType.MESH


def row_norm(values):
    return jnp.sqrt(1.0 + jnp.sum(values * values, axis=1, keepdims=True))


def sort_pairs(n):
    p = 1
    while p < n:
        k = p
        while k >= 1:
            for j in range(k % p, n - k, 2 * k):
                for i in range(min(k, n - j - k)):
                    if (i + j) // (2 * p) == (i + j + k) // (2 * p):
                        yield i + j, i + j + k
            k //= 2
        p *= 2


def sort_desc(v):
    v = list(v)
    for a, b in sort_pairs(len(v)):
        v[a], v[b] = jnp.maximum(v[a], v[b]), jnp.minimum(v[a], v[b])
    return v


def bitonic_desc(v):
    n = len(v)
    step = n // 2
    while step:
        for i in range(n):
            if not i & step:
                v[i], v[i + step] = jnp.maximum(v[i], v[i + step]), jnp.minimum(v[i], v[i + step])
        step //= 2
    return v


def merge_top(a, b):
    n = len(a)
    if n < TOPK:
        return bitonic_desc(a + b[::-1])
    return bitonic_desc([jnp.maximum(a[i], b[n - 1 - i]) for i in range(n)])


def search_kernel(
    q_hbm, pd_hbm, pl_hbm, sd_hbm, sl_hbm, sr_hbm, len_ref, docs_hbm, top_ref, short_ref, *scratch,
):
    chunks = q_hbm.shape[1] // WIDTH
    gathered = scratch[:chunks]
    (queries, pd, plist, sd, sl, sr, pre_docs, top_docs, unit, spots, chosen, result,
     ret, got, acc, part_ret, part_got, load_sem, send_sem, line_recv, cube_recv,
     top_sem, part_sem) = scratch[chunks:]
    gx, gy = lax.axis_index("gx"), lax.axis_index("gy")
    line = lax.axis_size("gy")
    bits = (lax.axis_size("gx") - 1).bit_length()
    ranks = 1 << bits
    lists, rows, full = docs_hbm.shape
    query_rows = q_hbm.shape[0]
    probes, shorts = pd.shape[1], sd.shape[1]
    count = ranks * line
    total = count * query_rows
    tiles = total // TILE
    per_tile = TILE // query_rows
    per_lane = LANES // query_rows
    packed = query_rows * TOPK // LANES
    me = (gx * line + gy).astype(jnp.float32)

    def cross(r):
        there = gx
        for b in range(bits):
            if r >> b & 1:
                there = there + (1 - 2 * ((gx // (1 << b)) % 2)) * (1 << b)
        return there

    def slot(r, k):
        return ((r & 1) * (ranks // 2) + (r >> 1)) * line + k

    places = sorted((slot(r, k), r, k) for r in range(ranks) for k in range(line))
    across = [cross(r) for r in range(ranks)]

    barrier = pltpu.get_barrier_semaphore()
    for k in range(1, line):
        pl.semaphore_signal(barrier, inc=1, device_id=(gx, (gy + k) % line), device_id_type=MESH)
    for b in range(bits):
        pl.semaphore_signal(barrier, inc=1, device_id=(across[1 << b], gy), device_id_type=MESH)

    first = pltpu.make_async_copy(q_hbm.at[:, pl.ds(0, WIDTH)], gathered[0].at[0, :, pl.ds(0, WIDTH)], load_sem.at[0])
    first.start()
    small = [
        pltpu.make_async_copy(src, dst, load_sem.at[1 + i])
        for i, (src, dst) in enumerate([(pd_hbm, pd), (pl_hbm, plist), (sd_hbm, sd), (sl_hbm, sl), (sr_hbm, sr)])
    ]
    for copy in small:
        copy.start()
    whole = pltpu.make_async_copy(q_hbm, queries, load_sem.at[6])
    whole.start()
    pre_copy = pltpu.make_async_copy(docs_hbm.at[:, :, pl.ds(0, PREFIX)], pre_docs, load_sem.at[7])
    top_copy = pltpu.make_async_copy(docs_hbm.at[:, pl.ds(0, SHORT_ROWS), :], top_docs, load_sem.at[8])
    pre_copy.start()
    top_copy.start()
    for copy in small:
        copy.wait()
    codes = jnp.concatenate([x[...].astype(jnp.float32) for x in (pd, plist, sd, sl, sr)], axis=1)
    gathered[0][0, :, WIDTH:] = codes.astype(jnp.bfloat16)
    whole.wait()
    values = queries[...].astype(jnp.float32)
    norm = row_norm(values)
    for c in range(1, chunks):
        gathered[c][0] = (values[:, c * WIDTH:(c + 1) * WIDTH] / norm).astype(jnp.bfloat16)
    first.wait()
    pl.semaphore_wait(barrier, line - 1 + bits)

    def order(c):
        inner = list(range(1, bits))
        return inner if c % 2 == 0 else inner[::-1]

    def push(c, source, target, n, recv, device):
        pltpu.make_async_remote_copy(
            src_ref=gathered[c].at[pl.ds(source, n)], dst_ref=gathered[c].at[pl.ds(target, n)],
            send_sem=send_sem.at[c], recv_sem=recv, device_id=device, device_id_type=MESH,
        ).start()

    def pushes(c, r, k, n, stage):
        for b in order(c)[stage:]:
            push(c, slot(r, k), slot(r | 1 << b, k), n, cube_recv.at[c, b], (across[1 << b], gy))

    def arrived(ref, n, sem):
        part = ref.at[pl.ds(0, n)]
        pltpu.make_async_copy(part, part, sem).wait()

    def begin(c):
        for k in range(1, line):
            push(c, 0, k, 1, line_recv.at[c], (gx, (gy + k) % line))
        pushes(c, 0, 0, 1, 0)

    def relay(c, stage):
        inner = order(c)
        if stage == 0:
            arrived(gathered[c], line - 1, line_recv.at[c])
            pushes(c, 0, 1, line - 1, 0)
        else:
            b = inner[stage - 1]
            free = inner[:stage - 1]
            arrived(gathered[c], line << len(free), cube_recv.at[c, b])
            for pick in range(1 << len(free)):
                r = 1 << b
                for i, f in enumerate(free):
                    if pick >> i & 1:
                        r |= 1 << f
                pushes(c, r, 0, line, stage)
        if stage == len(inner):
            push(c, 0, count // 2, count // 2, cube_recv.at[c, 0], (across[1], gy))

    def rows_of(c, t, lo, hi):
        return gathered[c][t * per_tile:(t + 1) * per_tile, :, lo:hi].reshape(TILE, hi - lo)

    def give_tops(t):
        lane = lax.broadcasted_iota(jnp.int32, (8, LANES), 1)
        for u in range(TILE // LANES):
            turned = jnp.transpose(result[:, u * LANES:(u + 1) * LANES])
            for i in range(per_lane):
                low = turned[i * query_rows:i * query_rows + 8]
                high = pltpu.roll(turned[i * query_rows + 8:(i + 1) * query_rows], 64, 1)
                pair = jnp.where(lane < 64, low, high)
                swapped = pltpu.roll(pltpu.roll(pair, 4, 0), TOPK, 1)
                message = jnp.where(lane % 64 < TOPK, pair, swapped)[:packed]
                s, r, k = places[t * per_tile + u * per_lane + i]
                if s == 0:
                    got[0] = message
                    continue
                ret[s] = message
                pltpu.make_async_remote_copy(
                    src_ref=ret.at[s], dst_ref=got.at[s], send_sem=top_sem.at[0], recv_sem=top_sem.at[1],
                    device_id=(across[r], (gy + line - k) % line), device_id_type=MESH,
                ).start()

    def prefix(t):
        lanes = slice(t * TILE, (t + 1) * TILE)
        raw = rows_of(0, t, 0, PREFIX).astype(jnp.float32)
        unit[lanes, :] = (raw / row_norm(raw)).astype(jnp.bfloat16)
        turned = jnp.transpose(rows_of(0, t, WIDTH, WIDTH + LANES).astype(jnp.float32))
        p_dev, p_list = turned[:probes], turned[probes:2 * probes]
        base = 2 * probes
        s_dev, s_list, s_row = (turned[base + i * shorts:base + (i + 1) * shorts] for i in range(3))
        probed = jnp.sum(jnp.where(p_dev == me, p_list + 1.0, 0.0), axis=0, keepdims=True).astype(jnp.int32) - 1
        at = s_list * SHORT_ROWS + s_row + 1.0
        wanted = jnp.sum(jnp.where(s_dev == me, at, 0.0), axis=0, keepdims=True).astype(jnp.int32) - 1
        spots[0:1, lanes] = wanted
        chunk = 32

        @pl.loop(0, rows // chunk)
        def _(c):
            start = pl.multiple_of(c * chunk, chunk)
            docs = pre_docs[:, pl.ds(start, chunk), :].reshape(lists * chunk, PREFIX)
            scores = lax.dot_general(docs, unit[lanes, :], NT, preferred_element_type=jnp.float32)
            place = lax.broadcasted_iota(jnp.int32, (chunk, TILE), 0) + start
            value = jnp.full((chunk, TILE), -jnp.inf, jnp.float32)
            for l in range(lists):
                limit = jnp.where(probed == l, len_ref[l], 0)
                value = jnp.where(place < limit, scores[l * chunk:(l + 1) * chunk], value)
            chosen[pl.ds(start, chunk), :] = value

        @pl.loop(0, TILE // LANES)
        def _(u):
            spot = pl.ds(pl.multiple_of(u * LANES, LANES), LANES)
            v = [chosen[pl.ds(8 * i, 8), spot] for i in range(rows // 8)]
            parts = [sort_desc(v[i:i + TOPK]) for i in range(0, len(v), TOPK)]
            v = functools.reduce(merge_top, parts)
            for shift in (4, 2, 1):
                v = merge_top(v, [pltpu.roll(x, shift, 0) for x in v])
            sub = lax.broadcasted_iota(jnp.int32, (8, LANES), 0)
            for a in range(TOPK // 8):
                one = v[8 * a]
                for s in range(1, 8):
                    one = jnp.where(sub == s, v[8 * a + s], one)
                result[pl.ds(8 * a, 8), spot] = one

        give_tops(t)

    group = 4

    def rescore(c, t):
        lanes = slice(t * TILE, (t + 1) * TILE)
        block = rows_of(c, t, 0, WIDTH)
        wanted = spots[0:1, lanes]
        place = lax.broadcasted_iota(jnp.int32, (SHORT_ROWS, TILE), 0)
        kind = 0 if c == 0 else 1

        def step(g, total_acc):
            docs = top_docs[pl.ds(g * group, group), :, c * WIDTH:(c + 1) * WIDTH].reshape(group * SHORT_ROWS, WIDTH)
            scores = lax.dot_general(docs, block, NT, preferred_element_type=jnp.float32)
            for j in range(group):
                hit = place == wanted - (g * group + j) * SHORT_ROWS
                part = jnp.where(hit, scores[j * SHORT_ROWS:(j + 1) * SHORT_ROWS], 0.0)
                total_acc = total_acc + jnp.sum(part.reshape(SHORT_ROWS // 8, 8, TILE), axis=0)
            return total_acc

        before = jnp.zeros((8, TILE), jnp.float32) if c < 2 else acc[kind, :, lanes]
        acc[kind, :, lanes] = lax.fori_loop(0, lists // group, step, before)

    def work(c):
        if c == 0:
            pre_copy.wait()
            for t in range(tiles):
                prefix(t)
            top_copy.wait()
        for t in range(tiles):
            rescore(c, t)

    for c in range(chunks):
        begin(c)
    depth = bits + 1
    for wave in range(chunks + depth):
        for stage in range(depth, -1, -1):
            c = wave - stage
            if not 0 <= c < chunks:
                continue
            if stage < bits:
                relay(c, stage)
            elif stage == bits:
                arrived(gathered[c], count // 2, cube_recv.at[c, 0])
                work(c)

    for kind in range(2):
        sums = jnp.sum(acc[kind], axis=0, keepdims=True)
        for g in range(total // LANES):
            part_ret[g, kind:kind + 1, :] = sums[:, g * LANES:(g + 1) * LANES]
    part_got[0] = part_ret[0]
    for s, r, k in places[1:]:
        pltpu.make_async_remote_copy(
            src_ref=part_ret.at[s // per_lane], dst_ref=part_got.at[s], send_sem=part_sem.at[0],
            recv_sem=part_sem.at[1], device_id=(across[r], (gy + line - k) % line), device_id_type=MESH,
        ).start()

    arrived(got, count - 1, top_sem.at[1])
    v = [jnp.concatenate([got[i], got[i + 1]], axis=0) for i in range(0, count, 2)]
    parts = [sort_desc(v[i:i + TOPK]) for i in range(0, len(v), TOPK)]
    best = functools.reduce(merge_top, parts)
    best = merge_top(best, [pltpu.roll(x, 4, 0) for x in best])
    shift = TOPK // 2
    while shift:
        best = merge_top(best, [pltpu.roll(x, LANES - shift, 1) for x in best])
        shift //= 2
    lane = lax.broadcasted_iota(jnp.int32, (8, LANES), 1)
    out = best[0]
    for i in range(1, TOPK):
        out = jnp.where(lane % TOPK == i, pltpu.roll(best[i], i, 1), out)
    for g in range(LANES // TOPK):
        moved = out if g == 0 else pltpu.roll(out, LANES - g * TOPK, 1)
        top_ref[g * packed:(g + 1) * packed, :] = moved[:packed, :TOPK]

    arrived(part_got, count - 1, part_sem.at[1])
    lane = lax.broadcasted_iota(jnp.int32, (count, LANES), 1)
    owner = lax.broadcasted_iota(jnp.int32, (count, LANES), 0) % per_lane
    sums = []
    for kind in range(2):
        kept = jnp.where(lane // query_rows == owner, part_got[:, kind, :], 0.0)
        sums.append(jnp.sum(jnp.transpose(kept).reshape(per_lane, query_rows, count), axis=0))
    rescored = sums[0] / norm + sums[1]
    dev = sd[...]
    picked = jnp.zeros((query_rows, shorts), jnp.float32)
    for s, r, k in places:
        there = across[r] * line + (gy + k) % line
        picked = jnp.where(dev == there, rescored[:, s:s + 1], picked)
    short_ref[...] = picked

    for c in range(chunks):
        arrived(gathered[c], count - 1, send_sem.at[c])
    arrived(got, count - 1, top_sem.at[0])
    arrived(part_got, count - 1, part_sem.at[0])


def shards(queries, probe_dev, probe_list, documents, lengths, short_dev, short_list, short_row):
    count = lax.axis_size(AXES)
    lists, rows, full = documents.shape
    query_rows = queries.shape[0]
    probes, shorts = probe_dev.shape[1], short_dev.shape[1]
    total = count * query_rows
    chunks = full // WIDTH
    bits = (lax.axis_size("gx") - 1).bit_length()
    packed = query_rows * TOPK // LANES
    extra = 2 * probes + 3 * shorts
    vmem = pl.BlockSpec(memory_space=pltpu.VMEM)
    hbm = pl.BlockSpec(memory_space=pl.ANY)
    dma = pltpu.SemaphoreType.DMA
    return pl.pallas_call(
        search_kernel,
        out_shape=(
            jax.ShapeDtypeStruct((query_rows, TOPK), jnp.float32),
            jax.ShapeDtypeStruct((query_rows, shorts), jnp.float32),
        ),
        in_specs=[hbm] * 6 + [pl.BlockSpec(memory_space=pltpu.SMEM), hbm],
        out_specs=(vmem, vmem),
        scratch_shapes=[
            pltpu.VMEM((count, query_rows, WIDTH + (extra if c == 0 else 0)), jnp.bfloat16) for c in range(chunks)
        ] + [
            pltpu.VMEM((query_rows, full), jnp.bfloat16),
            pltpu.VMEM((query_rows, probes), jnp.int32),
            pltpu.VMEM((query_rows, probes), jnp.int32),
            pltpu.VMEM((query_rows, shorts), jnp.int32),
            pltpu.VMEM((query_rows, shorts), jnp.int32),
            pltpu.VMEM((query_rows, shorts), jnp.int32),
            pltpu.VMEM((lists, rows, PREFIX), jnp.bfloat16),
            pltpu.VMEM((lists, SHORT_ROWS, full), jnp.bfloat16),
            pltpu.VMEM((total, PREFIX), jnp.bfloat16),
            pltpu.VMEM((8, total), jnp.int32),
            pltpu.VMEM((rows, TILE), jnp.float32),
            pltpu.VMEM((LANES, TILE), jnp.float32),
            pltpu.VMEM((count, packed, LANES), jnp.float32),
            pltpu.VMEM((count, packed, LANES), jnp.float32),
            pltpu.VMEM((2, 8, total), jnp.float32),
            pltpu.VMEM((total // LANES, 2, LANES), jnp.float32),
            pltpu.VMEM((count, 2, LANES), jnp.float32),
            dma((9,)),
            dma((chunks,)),
            dma((chunks,)),
            dma((chunks, bits)),
            dma((2,)),
            dma((2,)),
        ],
        compiler_params=pltpu.CompilerParams(
            collective_id=0, has_side_effects=True, vmem_limit_bytes=60 * 1024 * 1024
        ),
        name="search",
    )(queries, probe_dev, probe_list, short_dev, short_list, short_row, lengths, documents)


def solution(mesh):
    one = P(AXES, None)
    in_specs = (one, one, one, P(AXES, None, None), P(AXES), one, one, one)
    return jax.shard_map(shards, mesh=mesh, in_specs=in_specs, out_specs=(one, one), check_vma=False)
```

```python
import functools

import jax
import jax.numpy as jnp
from jax import lax
from jax.experimental import pallas as pl
from jax.experimental.pallas import tpu as pltpu
from jax.sharding import PartitionSpec as P

PREFIX = 256
TOPK = 32
SHORT_ROWS = 96
AXES = ("gx", "gy")
LANES = 128
TILE = 256
NT = (((1,), (1,)), ((), ()))
MESH = pl.DeviceIdType.MESH


def row_norm(values):
    return jnp.sqrt(1.0 + jnp.sum(values * values, axis=1, keepdims=True))


def sort_pairs(n):
    p = 1
    while p < n:
        k = p
        while k >= 1:
            for j in range(k % p, n - k, 2 * k):
                for i in range(min(k, n - j - k)):
                    if (i + j) // (2 * p) == (i + j + k) // (2 * p):
                        yield i + j, i + j + k
            k //= 2
        p *= 2


def sort_desc(v):
    v = list(v)
    for a, b in sort_pairs(len(v)):
        v[a], v[b] = jnp.maximum(v[a], v[b]), jnp.minimum(v[a], v[b])
    return v


def bitonic_desc(v):
    n = len(v)
    step = n // 2
    while step:
        for i in range(n):
            if not i & step:
                v[i], v[i + step] = jnp.maximum(v[i], v[i + step]), jnp.minimum(v[i], v[i + step])
        step //= 2
    return v


def merge_top(a, b):
    n = len(a)
    if n < TOPK:
        return bitonic_desc(a + b[::-1])
    return bitonic_desc([jnp.maximum(a[i], b[n - 1 - i]) for i in range(n)])


def column_cuts(full):
    cuts = [0, PREFIX]
    while full - cuts[-1] > 2 * PREFIX:
        cuts.append(cuts[-1] + 2 * PREFIX)
    return cuts + [full]


def search_kernel(
    q_hbm, pd_hbm, pl_hbm, sd_hbm, sl_hbm, sr_hbm, len_ref, docs_hbm, out_ref, *scratch,
):
    cuts = column_cuts(q_hbm.shape[1])
    chunks = len(cuts) - 1
    gathered = scratch[:chunks]
    (queries, pd, plist, sd, sl, sr, pre_docs, top_docs, unit, spots, chosen, result,
     ret, got, acc, part_ret, part_got, load_sem, send_sem, line_recv, plane_recv, core_recv,
     top_sem, part_sem) = scratch[chunks:]
    gx, gy = lax.axis_index("gx"), lax.axis_index("gy")
    line = lax.axis_size("gy")
    bits = (lax.axis_size("gx") - 1).bit_length()
    ranks = 1 << bits
    lists, rows, full = docs_hbm.shape
    query_rows = q_hbm.shape[0]
    probes, shorts = pd.shape[1], sd.shape[1]
    count = ranks * line
    total = count * query_rows
    tiles = total // TILE
    per_tile = TILE // query_rows
    per_lane = LANES // query_rows
    packed = query_rows * TOPK // LANES
    me = (gx * line + gy).astype(jnp.float32)

    def cross(r):
        there = gx
        for b in range(bits):
            if r >> b & 1:
                there = there + (1 - 2 * ((gx // (1 << b)) % 2)) * (1 << b)
        return there

    def slot(r, k):
        return ((r & 1) * (ranks // 2) + (r >> 1)) * line + k

    places = sorted((slot(r, k), r, k) for r in range(ranks) for k in range(line))
    across = [cross(r) for r in range(ranks)]

    barrier = pltpu.get_barrier_semaphore()
    for k in range(1, line):
        pl.semaphore_signal(barrier, inc=1, device_id=(gx, (gy + k) % line), device_id_type=MESH)
    for r in [1, *range(2, ranks, 2)]:
        pl.semaphore_signal(barrier, inc=1, device_id=(across[r], gy), device_id_type=MESH)

    first = pltpu.make_async_copy(q_hbm.at[:, pl.ds(0, PREFIX)], gathered[0].at[0, :, pl.ds(0, PREFIX)], load_sem.at[0])
    first.start()
    small = [
        pltpu.make_async_copy(src, dst, load_sem.at[1 + i])
        for i, (src, dst) in enumerate([(pd_hbm, pd), (pl_hbm, plist), (sd_hbm, sd), (sl_hbm, sl), (sr_hbm, sr)])
    ]
    for copy in small:
        copy.start()
    whole = pltpu.make_async_copy(q_hbm, queries, load_sem.at[6])
    whole.start()
    pre_copy = pltpu.make_async_copy(docs_hbm.at[:, :, pl.ds(0, PREFIX)], pre_docs, load_sem.at[7])
    top_copy = pltpu.make_async_copy(docs_hbm.at[:, pl.ds(0, SHORT_ROWS), :], top_docs, load_sem.at[8])
    pre_copy.start()
    top_copy.start()
    for copy in small:
        copy.wait()
    codes = jnp.concatenate([x[...].astype(jnp.float32) for x in (pd, plist, sd, sl, sr)], axis=1)
    gathered[0][0, :, PREFIX:] = codes.astype(jnp.bfloat16)
    first.wait()
    pl.semaphore_wait(barrier, line + ranks // 2 - 1)
    plane = [r for r in range(2, ranks, 2)]

    def push(c, source, target, n, recv, device):
        pltpu.make_async_remote_copy(
            src_ref=gathered[c].at[pl.ds(source, n)], dst_ref=gathered[c].at[pl.ds(target, n)],
            send_sem=send_sem.at[c], recv_sem=recv, device_id=device, device_id_type=MESH,
        ).start()

    def arrived(ref, n, sem):
        part = ref.at[pl.ds(0, n)]
        pltpu.make_async_copy(part, part, sem).wait()

    def begin(c):
        for k in range(1, line):
            push(c, 0, k, 1, line_recv.at[c], (gx, (gy + k) % line))
        for r in plane:
            push(c, 0, slot(r, 0), 1, plane_recv.at[c], (across[r], gy))

    def spread(c):
        arrived(gathered[c], line - 1, line_recv.at[c])
        for r in plane:
            push(c, 1, slot(r, 1), line - 1, plane_recv.at[c], (across[r], gy))

    def share(c):
        arrived(gathered[c], len(plane) * line, plane_recv.at[c])
        push(c, 0, count // 2, count // 2, core_recv.at[c], (across[1], gy))

    def shared(c):
        arrived(gathered[c], count // 2, core_recv.at[c])

    begin(0)
    whole.wait()
    values = queries[...].astype(jnp.float32)
    norm = row_norm(values)
    for c in range(1, chunks):
        gathered[c][0] = (values[:, cuts[c]:cuts[c + 1]] / norm).astype(jnp.bfloat16)
    for c in range(1, chunks):
        begin(c)

    def rows_of(c, t, lo, hi):
        return gathered[c][t * per_tile:(t + 1) * per_tile, :, lo:hi].reshape(TILE, hi - lo)

    def pack_tops(t):
        lane = lax.broadcasted_iota(jnp.int32, (8, LANES), 1)
        for u in range(TILE // LANES):
            turned = jnp.transpose(result[:, u * LANES:(u + 1) * LANES])
            for i in range(per_lane):
                low = turned[i * query_rows:i * query_rows + 8]
                high = pltpu.roll(turned[i * query_rows + 8:(i + 1) * query_rows], 64, 1)
                pair = jnp.where(lane < 64, low, high)
                swapped = pltpu.roll(pltpu.roll(pair, 4, 0), TOPK, 1)
                message = jnp.where(lane % 64 < TOPK, pair, swapped)[:packed]
                s = t * per_tile + u * per_lane + i
                if s == 0:
                    got[0] = message
                else:
                    ret[s] = message

    def give(source, target, sems, some):
        for s, r, k in places[some.start * per_tile:some.stop * per_tile]:
            if s == 0:
                continue
            pltpu.make_async_remote_copy(
                src_ref=source(s), dst_ref=target.at[s], send_sem=sems.at[0], recv_sem=sems.at[1],
                device_id=(across[r], (gy + line - k) % line), device_id_type=MESH,
            ).start()

    def give_parts(some):
        lanes = slice(some.start * TILE, some.stop * TILE)
        first = some.start * TILE // LANES
        for kind in range(2):
            sums = jnp.sum(acc[kind, :, lanes], axis=0, keepdims=True)
            for g in range(len(some) * TILE // LANES):
                part_ret[first + g, kind:kind + 1, :] = sums[:, g * LANES:(g + 1) * LANES]
        if some.start == 0:
            part_got[0] = part_ret[0]
        give(lambda s: part_ret.at[s // per_lane], part_got, part_sem, some)

    def prefix(t):
        lanes = slice(t * TILE, (t + 1) * TILE)
        raw = rows_of(0, t, 0, PREFIX).astype(jnp.float32)
        unit[lanes, :] = (raw / row_norm(raw)).astype(jnp.bfloat16)
        turned = jnp.transpose(rows_of(0, t, PREFIX, gathered[0].shape[2]).astype(jnp.float32))
        p_dev, p_list = turned[:probes], turned[probes:2 * probes]
        base = 2 * probes
        s_dev, s_list, s_row = (turned[base + i * shorts:base + (i + 1) * shorts] for i in range(3))
        probed = jnp.sum(jnp.where(p_dev == me, p_list + 1.0, 0.0), axis=0, keepdims=True).astype(jnp.int32) - 1
        at = s_list * SHORT_ROWS + s_row + 1.0
        wanted = jnp.sum(jnp.where(s_dev == me, at, 0.0), axis=0, keepdims=True).astype(jnp.int32) - 1
        spots[0:1, lanes] = wanted
        chunk = 128

        @pl.loop(0, rows // chunk)
        def _(c):
            start = pl.multiple_of(c * chunk, chunk)
            docs = pre_docs[:, pl.ds(start, chunk), :].reshape(lists * chunk, PREFIX)
            scores = lax.dot_general(docs, unit[lanes, :], NT, preferred_element_type=jnp.float32)
            place = lax.broadcasted_iota(jnp.int32, (chunk, TILE), 0) + start
            value = jnp.full((chunk, TILE), -jnp.inf, jnp.float32)
            for l in range(lists):
                limit = jnp.where(probed == l, len_ref[l], 0)
                value = jnp.where(place < limit, scores[l * chunk:(l + 1) * chunk], value)
            chosen[pl.ds(start, chunk), :] = value

        @pl.loop(0, TILE // LANES)
        def _(u):
            spot = pl.ds(pl.multiple_of(u * LANES, LANES), LANES)
            v = [chosen[pl.ds(8 * i, 8), spot] for i in range(rows // 8)]
            parts = [sort_desc(v[i:i + TOPK]) for i in range(0, len(v), TOPK)]
            v = functools.reduce(merge_top, parts)
            for shift in (4, 2, 1):
                v = merge_top(v, [pltpu.roll(x, shift, 0) for x in v])
            sub = lax.broadcasted_iota(jnp.int32, (8, LANES), 0)
            for a in range(TOPK // 8):
                one = v[8 * a]
                for s in range(1, 8):
                    one = jnp.where(sub == s, v[8 * a + s], one)
                result[pl.ds(8 * a, 8), spot] = one

        pack_tops(t)

    def rescore(c, t):
        lanes = slice(t * TILE, (t + 1) * TILE)
        width = cuts[c + 1] - cuts[c]
        wanted = spots[0:1, lanes]
        place = lax.broadcasted_iota(jnp.int32, (SHORT_ROWS, TILE), 0)
        kind = 0 if c == 0 else 1
        docs = top_docs[:, :, cuts[c]:cuts[c + 1]].reshape(lists * SHORT_ROWS, width)
        scores = lax.dot_general(docs, rows_of(c, t, 0, width), NT, preferred_element_type=jnp.float32)
        sums = jnp.zeros((8, TILE), jnp.float32) if c < 2 else acc[kind, :, lanes]
        for j in range(lists):
            hit = place == wanted - j * SHORT_ROWS
            part = jnp.where(hit, scores[j * SHORT_ROWS:(j + 1) * SHORT_ROWS], 0.0)
            sums = sums + jnp.sum(part.reshape(SHORT_ROWS // 8, 8, TILE), axis=0)
        acc[kind, :, lanes] = sums

    halves = (range(tiles // 2), range(tiles // 2, tiles))
    for c in range(chunks):
        spread(c)
    share(0)
    pre_copy.wait()
    for t in halves[0]:
        prefix(t)
    shared(0)
    for t in halves[1]:
        prefix(t)
    top_copy.wait()
    for t in range(tiles):
        rescore(0, t)
    last = chunks - 1
    share(1)
    for c in range(1, chunks):
        for t in halves[0]:
            rescore(c, t)
        if c == last:
            give_parts(halves[0])
        elif c > 1:
            share(c + 1)
        if c == last - 2:
            give(lambda s: ret.at[s], got, top_sem, range(tiles))
        shared(c)
        for t in halves[1]:
            rescore(c, t)
        if c == 1:
            share(2)
    give_parts(halves[1])

    arrived(got, count - 1, top_sem.at[1])
    v = [jnp.concatenate([got[i], got[i + 1]], axis=0) for i in range(0, count, 2)]
    parts = [sort_desc(v[i:i + TOPK]) for i in range(0, len(v), TOPK)]
    best = functools.reduce(merge_top, parts)
    best = merge_top(best, [pltpu.roll(x, 4, 0) for x in best])
    shift = TOPK // 2
    while shift:
        best = merge_top(best, [pltpu.roll(x, LANES - shift, 1) for x in best])
        shift //= 2
    lane = lax.broadcasted_iota(jnp.int32, (8, LANES), 1)
    out = best[0]
    for i in range(1, TOPK):
        out = jnp.where(lane % TOPK == i, pltpu.roll(best[i], i, 1), out)
    for g in range(LANES // TOPK):
        moved = out if g == 0 else pltpu.roll(out, LANES - g * TOPK, 1)
        out_ref[g * packed:(g + 1) * packed, :TOPK] = moved[:packed, :TOPK]

    arrived(part_got, count - 1, part_sem.at[1])
    lane = lax.broadcasted_iota(jnp.int32, (count, LANES), 1)
    owner = lax.broadcasted_iota(jnp.int32, (count, LANES), 0) % per_lane
    sums = []
    for kind in range(2):
        kept = jnp.where(lane // query_rows == owner, part_got[:, kind, :], 0.0)
        sums.append(jnp.sum(jnp.transpose(kept).reshape(per_lane, query_rows, count), axis=0))
    rescored = sums[0] / norm + sums[1]
    dev = sd[...]
    picked = jnp.zeros((query_rows, shorts), jnp.float32)
    for s, r, k in places:
        there = across[r] * line + (gy + k) % line
        picked = jnp.where(dev == there, rescored[:, s:s + 1], picked)
    out_ref[:, TOPK:] = picked

    for c in range(chunks):
        arrived(gathered[c], count - 1, send_sem.at[c])
    arrived(got, count - 1, top_sem.at[0])
    arrived(part_got, count - 1, part_sem.at[0])


def shards(queries, probe_dev, probe_list, documents, lengths, short_dev, short_list, short_row):
    count = lax.axis_size(AXES)
    lists, rows, full = documents.shape
    query_rows = queries.shape[0]
    probes, shorts = probe_dev.shape[1], short_dev.shape[1]
    total = count * query_rows
    cuts = column_cuts(full)
    chunks = len(cuts) - 1
    packed = query_rows * TOPK // LANES
    extra = 2 * probes + 3 * shorts
    vmem = pl.BlockSpec(memory_space=pltpu.VMEM)
    hbm = pl.BlockSpec(memory_space=pl.ANY)
    dma = pltpu.SemaphoreType.DMA
    out = pl.pallas_call(
        search_kernel,
        out_shape=jax.ShapeDtypeStruct((query_rows, TOPK + shorts), jnp.float32),
        in_specs=[hbm] * 6 + [pl.BlockSpec(memory_space=pltpu.SMEM), hbm],
        out_specs=vmem,
        scratch_shapes=[
            pltpu.VMEM((count, query_rows, cuts[c + 1] - cuts[c] + (extra if c == 0 else 0)), jnp.bfloat16)
            for c in range(chunks)
        ] + [
            pltpu.VMEM((query_rows, full), jnp.bfloat16),
            pltpu.VMEM((query_rows, probes), jnp.int32),
            pltpu.VMEM((query_rows, probes), jnp.int32),
            pltpu.VMEM((query_rows, shorts), jnp.int32),
            pltpu.VMEM((query_rows, shorts), jnp.int32),
            pltpu.VMEM((query_rows, shorts), jnp.int32),
            pltpu.VMEM((lists, rows, PREFIX), jnp.bfloat16),
            pltpu.VMEM((lists, SHORT_ROWS, full), jnp.bfloat16),
            pltpu.VMEM((total, PREFIX), jnp.bfloat16),
            pltpu.VMEM((8, total), jnp.int32),
            pltpu.VMEM((rows, TILE), jnp.float32),
            pltpu.VMEM((LANES, TILE), jnp.float32),
            pltpu.VMEM((count, packed, LANES), jnp.float32),
            pltpu.VMEM((count, packed, LANES), jnp.float32),
            pltpu.VMEM((2, 8, total), jnp.float32),
            pltpu.VMEM((total // LANES, 2, LANES), jnp.float32),
            pltpu.VMEM((count, 2, LANES), jnp.float32),
            dma((9,)),
            dma((chunks,)),
            dma((chunks,)),
            dma((chunks,)),
            dma((chunks,)),
            dma((2,)),
            dma((2,)),
        ],
        compiler_params=pltpu.CompilerParams(
            collective_id=0, has_side_effects=True, vmem_limit_bytes=60 * 1024 * 1024
        ),
        name="search",
    )(queries, probe_dev, probe_list, short_dev, short_list, short_row, lengths, documents)
    return out[:, :TOPK], out[:, TOPK:]


def solution(mesh):
    one = P(AXES, None)
    in_specs = (one, one, one, P(AXES, None, None), P(AXES), one, one, one)
    return jax.shard_map(shards, mesh=mesh, in_specs=in_specs, out_specs=(one, one), check_vma=False)
```

```python
import functools

import jax
import jax.numpy as jnp
from jax import lax
from jax.experimental import pallas as pl
from jax.experimental.pallas import tpu as pltpu
from jax.sharding import PartitionSpec as P

PREFIX = 256
TOPK = 32
SHORT_ROWS = 96
AXES = ("gx", "gy")
LANES = 128
TILE = 256
NT = (((1,), (1,)), ((), ()))
MESH = pl.DeviceIdType.MESH


def row_norm(values):
    return jnp.sqrt(1.0 + jnp.sum(values * values, axis=1, keepdims=True))


def sort_pairs(n):
    p = 1
    while p < n:
        k = p
        while k >= 1:
            for j in range(k % p, n - k, 2 * k):
                for i in range(min(k, n - j - k)):
                    if (i + j) // (2 * p) == (i + j + k) // (2 * p):
                        yield i + j, i + j + k
            k //= 2
        p *= 2


def sort_desc(v):
    v = list(v)
    for a, b in sort_pairs(len(v)):
        v[a], v[b] = jnp.maximum(v[a], v[b]), jnp.minimum(v[a], v[b])
    return v


def bitonic_desc(v):
    n = len(v)
    step = n // 2
    while step:
        for i in range(n):
            if not i & step:
                v[i], v[i + step] = jnp.maximum(v[i], v[i + step]), jnp.minimum(v[i], v[i + step])
        step //= 2
    return v


def merge_top(a, b):
    n = len(a)
    if n < TOPK:
        return bitonic_desc(a + b[::-1])
    return bitonic_desc([jnp.maximum(a[i], b[n - 1 - i]) for i in range(n)])


def column_cuts(full):
    cuts = [0, PREFIX]
    while full - cuts[-1] > 2 * PREFIX:
        cuts.append(cuts[-1] + 2 * PREFIX)
    return cuts + [full]


def search_kernel(
    q_hbm, pd_hbm, pl_hbm, sd_hbm, sl_hbm, sr_hbm, len_ref, docs_hbm, out_ref, *scratch,
):
    cuts = column_cuts(q_hbm.shape[1])
    chunks = len(cuts) - 1
    gathered = scratch[:chunks]
    (queries, pd, plist, sd, sl, sr, pre_docs, top_docs, unit, spots, chosen, result,
     ret, got, acc, part_ret, part_got, load_sem, docs_sem, send_sem, line_recv, plane_recv, core_recv,
     top_sem, part_sem) = scratch[chunks:]
    gx, gy = lax.axis_index("gx"), lax.axis_index("gy")
    line = lax.axis_size("gy")
    bits = (lax.axis_size("gx") - 1).bit_length()
    ranks = 1 << bits
    lists, rows, full = docs_hbm.shape
    query_rows = q_hbm.shape[0]
    probes, shorts = pd.shape[1], sd.shape[1]
    count = ranks * line
    total = count * query_rows
    tiles = total // TILE
    per_tile = TILE // query_rows
    per_lane = LANES // query_rows
    packed = query_rows * TOPK // LANES
    me = (gx * line + gy).astype(jnp.float32)

    def cross(r):
        there = gx
        for b in range(bits):
            if r >> b & 1:
                there = there + (1 - 2 * ((gx // (1 << b)) % 2)) * (1 << b)
        return there

    def slot(r, k):
        return ((r & 1) * (ranks // 2) + (r >> 1)) * line + k

    places = sorted((slot(r, k), r, k) for r in range(ranks) for k in range(line))
    across = [cross(r) for r in range(ranks)]

    barrier = pltpu.get_barrier_semaphore()
    for k in range(1, line):
        pl.semaphore_signal(barrier, inc=1, device_id=(gx, (gy + k) % line), device_id_type=MESH)
    for r in [1, *range(2, ranks, 2)]:
        pl.semaphore_signal(barrier, inc=1, device_id=(across[r], gy), device_id_type=MESH)

    def columns(k):
        return pl.ds(k * LANES, LANES)

    head = PREFIX // LANES
    firsts = [
        pltpu.make_async_copy(q_hbm.at[:, columns(k)], gathered[0].at[k, 0], load_sem.at[7 + k]) for k in range(head)
    ]
    for copy in firsts:
        copy.start()
    small = [
        pltpu.make_async_copy(src, dst, load_sem.at[i])
        for i, (src, dst) in enumerate([(pd_hbm, pd), (pl_hbm, plist), (sd_hbm, sd), (sl_hbm, sl), (sr_hbm, sr)])
    ]
    for copy in small:
        copy.start()
    whole = pltpu.make_async_copy(q_hbm, queries, load_sem.at[5])
    whole.start()
    pre_copies = [
        pltpu.make_async_copy(docs_hbm.at[:, :, columns(k)], pre_docs.at[k], docs_sem.at[k]) for k in range(head)
    ]
    top_copies = [
        pltpu.make_async_copy(docs_hbm.at[:, pl.ds(0, SHORT_ROWS), columns(k)], top_docs.at[k - head], docs_sem.at[k])
        for k in range(head, full // LANES)
    ]
    for copy in pre_copies + top_copies:
        copy.start()
    for copy in small:
        copy.wait()
    codes = jnp.concatenate([x[...].astype(jnp.float32) for x in (pd, plist, sd, sl, sr)], axis=1)
    for k in range(head, gathered[0].shape[0]):
        gathered[0][k, 0] = codes[:, (k - head) * LANES:(k - head + 1) * LANES].astype(jnp.bfloat16)
    for copy in firsts:
        copy.wait()
    pl.semaphore_wait(barrier, line + ranks // 2 - 1)
    plane = [r for r in range(2, ranks, 2)]

    def push(c, source, target, n, recv, device):
        pltpu.make_async_remote_copy(
            src_ref=gathered[c].at[:, pl.ds(source, n)], dst_ref=gathered[c].at[:, pl.ds(target, n)],
            send_sem=send_sem.at[c], recv_sem=recv, device_id=device, device_id_type=MESH,
        ).start()

    def finish(part, sem):
        pltpu.make_async_copy(part, part, sem).wait()

    def arrived(c, n, sem):
        finish(gathered[c].at[:, pl.ds(0, n)], sem)

    def begin(c):
        for k in range(1, line):
            push(c, 0, k, 1, line_recv.at[c], (gx, (gy + k) % line))
        for r in plane:
            push(c, 0, slot(r, 0), 1, plane_recv.at[c], (across[r], gy))

    def spread(c):
        arrived(c, line - 1, line_recv.at[c])
        for r in plane:
            push(c, 1, slot(r, 1), line - 1, plane_recv.at[c], (across[r], gy))

    def share(c):
        arrived(c, len(plane) * line, plane_recv.at[c])
        push(c, 0, count // 2, count // 2, core_recv.at[c], (across[1], gy))

    def shared(c):
        arrived(c, count // 2, core_recv.at[c])

    begin(0)
    whole.wait()
    values = queries[...].astype(jnp.float32)
    norm = row_norm(values)
    for c in range(1, chunks):
        for k in range(gathered[c].shape[0]):
            at = cuts[c] + k * LANES
            gathered[c][k, 0] = (values[:, at:at + LANES] / norm).astype(jnp.bfloat16)
    for c in range(1, chunks):
        begin(c)

    def rows_of(c, t, ks):
        slots = slice(t * per_tile, (t + 1) * per_tile)
        return jnp.concatenate([gathered[c][k, slots].reshape(TILE, LANES) for k in ks], axis=1)

    def pack_tops(t):
        lane = lax.broadcasted_iota(jnp.int32, (8, LANES), 1)
        for u in range(TILE // LANES):
            turned = jnp.transpose(result[:, u * LANES:(u + 1) * LANES])
            for i in range(per_lane):
                low = turned[i * query_rows:i * query_rows + 8]
                high = pltpu.roll(turned[i * query_rows + 8:(i + 1) * query_rows], 64, 1)
                pair = jnp.where(lane < 64, low, high)
                swapped = pltpu.roll(pltpu.roll(pair, 4, 0), TOPK, 1)
                message = jnp.where(lane % 64 < TOPK, pair, swapped)[:packed]
                s = t * per_tile + u * per_lane + i
                if s == 0:
                    got[0] = message
                else:
                    ret[s] = message

    def give(source, target, sems, some):
        for s, r, k in places[some.start * per_tile:some.stop * per_tile]:
            if s == 0:
                continue
            pltpu.make_async_remote_copy(
                src_ref=source(s), dst_ref=target.at[s], send_sem=sems.at[0], recv_sem=sems.at[1],
                device_id=(across[r], (gy + line - k) % line), device_id_type=MESH,
            ).start()

    def give_parts(some):
        lanes = slice(some.start * TILE, some.stop * TILE)
        first = some.start * TILE // LANES
        for kind in range(2):
            sums = jnp.sum(acc[kind, :, lanes], axis=0, keepdims=True)
            for g in range(len(some) * TILE // LANES):
                part_ret[first + g, kind:kind + 1, :] = sums[:, g * LANES:(g + 1) * LANES]
        if some.start == 0:
            part_got[0] = part_ret[0]
        give(lambda s: part_ret.at[s // per_lane], part_got, part_sem, some)

    def prefix(t):
        lanes = slice(t * TILE, (t + 1) * TILE)
        raw = rows_of(0, t, range(head)).astype(jnp.float32)
        unit[lanes, :] = (raw / row_norm(raw)).astype(jnp.bfloat16)
        turned = jnp.transpose(rows_of(0, t, range(head, gathered[0].shape[0])).astype(jnp.float32))
        p_dev, p_list = turned[:probes], turned[probes:2 * probes]
        base = 2 * probes
        s_dev, s_list, s_row = (turned[base + i * shorts:base + (i + 1) * shorts] for i in range(3))
        probed = jnp.sum(jnp.where(p_dev == me, p_list + 1.0, 0.0), axis=0, keepdims=True).astype(jnp.int32) - 1
        at = s_list * SHORT_ROWS + s_row + 1.0
        wanted = jnp.sum(jnp.where(s_dev == me, at, 0.0), axis=0, keepdims=True).astype(jnp.int32) - 1
        spots[0:1, lanes] = wanted
        chunk = 32

        order = [slice(r, r + chunk) for r in range(0, rows, chunk)]
        limits = [jnp.where(probed == l, len_ref[l], 0) for l in range(lists)]
        for part in (order[:len(order) // 2], order[len(order) // 2:]):
            docs = jnp.concatenate([
                jnp.concatenate([pre_docs[k, :, some].reshape(lists * chunk, LANES) for k in range(head)], axis=1)
                for some in part
            ], axis=0)
            scores = lax.dot_general(docs, unit[lanes, :], NT, preferred_element_type=jnp.float32)
            for i, some in enumerate(part):
                place = lax.broadcasted_iota(jnp.int32, (chunk, TILE), 0) + some.start
                value = jnp.full((chunk, TILE), -jnp.inf, jnp.float32)
                for l in range(lists):
                    at = (i * lists + l) * chunk
                    value = jnp.where(place < limits[l], scores[at:at + chunk], value)
                chosen[t, some, :] = value

    def tops(t):
        for u in range(TILE // LANES):
            spot = slice(u * LANES, (u + 1) * LANES)
            v = [chosen[t, 8 * i:8 * i + 8, spot] for i in range(rows // 8)]
            parts = [sort_desc(v[i:i + TOPK]) for i in range(0, len(v), TOPK)]
            v = functools.reduce(merge_top, parts)
            for shift in (4, 2, 1):
                v = merge_top(v, [pltpu.roll(x, shift, 0) for x in v])
            sub = lax.broadcasted_iota(jnp.int32, (8, LANES), 0)
            for a in range(TOPK // 8):
                one = v[8 * a]
                for s in range(1, 8):
                    one = jnp.where(sub == s, v[8 * a + s], one)
                result[8 * a:8 * a + 8, spot] = one
        pack_tops(t)

    def rescore(c, t):
        lanes = slice(t * TILE, (t + 1) * TILE)
        width = cuts[c + 1] - cuts[c]
        wanted = spots[0:1, lanes]
        place = lax.broadcasted_iota(jnp.int32, (SHORT_ROWS, TILE), 0)
        kind = 0 if c == 0 else 1
        ks = range(width // LANES)
        tall = [pre_docs[k, :, :SHORT_ROWS] if c == 0 else top_docs[cuts[c] // LANES - head + k] for k in ks]
        docs = jnp.concatenate([x.reshape(lists * SHORT_ROWS, LANES) for x in tall], axis=1)
        scores = lax.dot_general(docs, rows_of(c, t, ks), NT, preferred_element_type=jnp.float32)
        sums = jnp.zeros((8, TILE), jnp.float32) if c < 2 else acc[kind, :, lanes]
        for j in range(lists):
            hit = place == wanted - j * SHORT_ROWS
            part = jnp.where(hit, scores[j * SHORT_ROWS:(j + 1) * SHORT_ROWS], 0.0)
            sums = sums + jnp.sum(part.reshape(SHORT_ROWS // 8, 8, TILE), axis=0)
        acc[kind, :, lanes] = sums

    halves = (range(tiles // 2), range(tiles // 2, tiles))
    for c in range(chunks):
        spread(c)
    share(0)
    for copy in pre_copies:
        copy.wait()
    for t in halves[0]:
        prefix(t)
    shared(0)
    for t in halves[0]:
        tops(t)
    for t in halves[1]:
        prefix(t)
    share(1)
    for t in range(tiles):
        rescore(0, t)
    for t in halves[1]:
        tops(t)
    for copy in top_copies:
        copy.wait()
    for c in range(1, chunks):
        if c + 1 < chunks:
            share(c + 1)
        shared(c)
        for t in range(tiles):
            rescore(c, t)
        if c == chunks - 3:
            give(lambda s: ret.at[s], got, top_sem, range(tiles))
    give_parts(range(tiles))

    finish(got.at[pl.ds(0, count - 1)], top_sem.at[1])
    v = [jnp.concatenate([got[i], got[i + 1]], axis=0) for i in range(0, count, 2)]
    parts = [sort_desc(v[i:i + TOPK]) for i in range(0, len(v), TOPK)]
    best = functools.reduce(merge_top, parts)
    best = merge_top(best, [pltpu.roll(x, 4, 0) for x in best])
    shift = TOPK // 2
    while shift:
        best = merge_top(best, [pltpu.roll(x, LANES - shift, 1) for x in best])
        shift //= 2
    lane = lax.broadcasted_iota(jnp.int32, (8, LANES), 1)
    out = best[0]
    for i in range(1, TOPK):
        out = jnp.where(lane % TOPK == i, pltpu.roll(best[i], i, 1), out)
    for g in range(LANES // TOPK):
        moved = out if g == 0 else pltpu.roll(out, LANES - g * TOPK, 1)
        out_ref[g * packed:(g + 1) * packed, :TOPK] = moved[:packed, :TOPK]

    finish(part_got.at[pl.ds(0, count - 1)], part_sem.at[1])
    lane = lax.broadcasted_iota(jnp.int32, (count, LANES), 1)
    owner = lax.broadcasted_iota(jnp.int32, (count, LANES), 0) % per_lane
    sums = []
    for kind in range(2):
        kept = jnp.where(lane // query_rows == owner, part_got[:, kind, :], 0.0)
        sums.append(jnp.sum(jnp.transpose(kept).reshape(per_lane, query_rows, count), axis=0))
    rescored = sums[0] / norm + sums[1]
    dev = sd[...]
    picked = jnp.zeros((query_rows, shorts), jnp.float32)
    for s, r, k in places:
        there = across[r] * line + (gy + k) % line
        picked = jnp.where(dev == there, rescored[:, s:s + 1], picked)
    out_ref[:, TOPK:] = picked

    for c in range(chunks):
        arrived(c, count - 1, send_sem.at[c])
    finish(got.at[pl.ds(0, count - 1)], top_sem.at[0])
    finish(part_got.at[pl.ds(0, count - 1)], part_sem.at[0])


def shards(queries, probe_dev, probe_list, documents, lengths, short_dev, short_list, short_row):
    count = lax.axis_size(AXES)
    lists, rows, full = documents.shape
    query_rows = queries.shape[0]
    probes, shorts = probe_dev.shape[1], short_dev.shape[1]
    total = count * query_rows
    cuts = column_cuts(full)
    chunks = len(cuts) - 1
    packed = query_rows * TOPK // LANES
    extra = 2 * probes + 3 * shorts
    vmem = pl.BlockSpec(memory_space=pltpu.VMEM)
    hbm = pl.BlockSpec(memory_space=pl.ANY)
    dma = pltpu.SemaphoreType.DMA
    out = pl.pallas_call(
        search_kernel,
        out_shape=jax.ShapeDtypeStruct((query_rows, TOPK + shorts), jnp.float32),
        in_specs=[hbm] * 6 + [pl.BlockSpec(memory_space=pltpu.SMEM), hbm],
        out_specs=vmem,
        scratch_shapes=[
            pltpu.VMEM(
                ((cuts[c + 1] - cuts[c] + (extra if c == 0 else 0)) // LANES, count, query_rows, LANES), jnp.bfloat16
            )
            for c in range(chunks)
        ] + [
            pltpu.VMEM((query_rows, full), jnp.bfloat16),
            pltpu.VMEM((query_rows, probes), jnp.int32),
            pltpu.VMEM((query_rows, probes), jnp.int32),
            pltpu.VMEM((query_rows, shorts), jnp.int32),
            pltpu.VMEM((query_rows, shorts), jnp.int32),
            pltpu.VMEM((query_rows, shorts), jnp.int32),
            pltpu.VMEM((PREFIX // LANES, lists, rows, LANES), jnp.bfloat16),
            pltpu.VMEM(((full - PREFIX) // LANES, lists, SHORT_ROWS, LANES), jnp.bfloat16),
            pltpu.VMEM((total, PREFIX), jnp.bfloat16),
            pltpu.VMEM((8, total), jnp.int32),
            pltpu.VMEM((total // TILE, rows, TILE), jnp.float32),
            pltpu.VMEM((LANES, TILE), jnp.float32),
            pltpu.VMEM((count, packed, LANES), jnp.float32),
            pltpu.VMEM((count, packed, LANES), jnp.float32),
            pltpu.VMEM((2, 8, total), jnp.float32),
            pltpu.VMEM((total // LANES, 2, LANES), jnp.float32),
            pltpu.VMEM((count, 2, LANES), jnp.float32),
            dma((9,)),
            dma((full // LANES,)),
            dma((chunks,)),
            dma((chunks,)),
            dma((chunks,)),
            dma((chunks,)),
            dma((2,)),
            dma((2,)),
        ],
        compiler_params=pltpu.CompilerParams(
            collective_id=0, has_side_effects=True, vmem_limit_bytes=60 * 1024 * 1024
        ),
        name="search",
    )(queries, probe_dev, probe_list, short_dev, short_list, short_row, lengths, documents)
    return out[:, :TOPK], out[:, TOPK:]


def solution(mesh):
    one = P(AXES, None)
    in_specs = (one, one, one, P(AXES, None, None), P(AXES), one, one, one)
    return jax.shard_map(shards, mesh=mesh, in_specs=in_specs, out_specs=(one, one), check_vma=False)
```

```python
import functools

import jax
import jax.numpy as jnp
from jax import lax
from jax.experimental import pallas as pl
from jax.experimental.pallas import tpu as pltpu
from jax.sharding import PartitionSpec as P

PREFIX = 256
TOPK = 32
SHORT_ROWS = 96
AXES = ("gx", "gy")
LANES = 128
TILE = 256
NT = (((1,), (1,)), ((), ()))
MESH = pl.DeviceIdType.MESH


def row_norm(values):
    return jnp.sqrt(1.0 + jnp.sum(values * values, axis=1, keepdims=True))


def sort_pairs(n):
    p = 1
    while p < n:
        k = p
        while k >= 1:
            for j in range(k % p, n - k, 2 * k):
                for i in range(min(k, n - j - k)):
                    if (i + j) // (2 * p) == (i + j + k) // (2 * p):
                        yield i + j, i + j + k
            k //= 2
        p *= 2


def sort_desc(v):
    v = list(v)
    for a, b in sort_pairs(len(v)):
        v[a], v[b] = jnp.maximum(v[a], v[b]), jnp.minimum(v[a], v[b])
    return v


def bitonic_desc(v):
    n = len(v)
    step = n // 2
    while step:
        for i in range(n):
            if not i & step:
                v[i], v[i + step] = jnp.maximum(v[i], v[i + step]), jnp.minimum(v[i], v[i + step])
        step //= 2
    return v


def merge_top(a, b):
    n = len(a)
    if n < TOPK:
        return bitonic_desc(a + b[::-1])
    return bitonic_desc([jnp.maximum(a[i], b[n - 1 - i]) for i in range(n)])


def column_cuts(full):
    cuts = [0, PREFIX]
    while full - cuts[-1] > 2 * PREFIX:
        cuts.append(cuts[-1] + 2 * PREFIX)
    return cuts + [full]


def search_kernel(
    q_hbm, pd_hbm, pl_hbm, sd_hbm, sl_hbm, sr_hbm, len_hbm, docs_hbm, out_ref, *scratch,
):
    cuts = column_cuts(q_hbm.shape[1])
    chunks = len(cuts) - 1
    gathered = scratch[:chunks]
    (queries, len_ref, pd, plist, sd, sl, sr, pre_docs, top_docs, unit, spots, chosen, result,
     ret, got, acc, part_ret, part_got, load_sem, docs_sem, send_sem, line_recv, plane_recv, core_recv,
     top_sem, part_sem) = scratch[chunks:]
    gx, gy = lax.axis_index("gx"), lax.axis_index("gy")
    line = lax.axis_size("gy")
    bits = (lax.axis_size("gx") - 1).bit_length()
    ranks = 1 << bits
    lists, rows, full = docs_hbm.shape
    query_rows = q_hbm.shape[0]
    probes, shorts = pd.shape[1], sd.shape[1]
    count = ranks * line
    total = count * query_rows
    tiles = total // TILE
    per_tile = TILE // query_rows
    per_lane = LANES // query_rows
    packed = query_rows * TOPK // LANES
    me = (gx * line + gy).astype(jnp.float32)

    def cross(r):
        there = gx
        for b in range(bits):
            if r >> b & 1:
                there = there + (1 - 2 * ((gx // (1 << b)) % 2)) * (1 << b)
        return there

    def slot(r, k):
        return ((r & 1) * (ranks // 2) + (r >> 1)) * line + k

    places = sorted((slot(r, k), r, k) for r in range(ranks) for k in range(line))
    across = [cross(r) for r in range(ranks)]

    barrier = pltpu.get_barrier_semaphore()
    for k in range(1, line):
        pl.semaphore_signal(barrier, inc=1, device_id=(gx, (gy + k) % line), device_id_type=MESH)
    for r in [1, *range(2, ranks, 2)]:
        pl.semaphore_signal(barrier, inc=1, device_id=(across[r], gy), device_id_type=MESH)

    def columns(k):
        return pl.ds(k * LANES, LANES)

    head = PREFIX // LANES
    firsts = [
        pltpu.make_async_copy(q_hbm.at[:, columns(k)], gathered[0].at[k, 0], load_sem.at[7 + k]) for k in range(head)
    ]
    for copy in firsts:
        copy.start()
    small = [
        pltpu.make_async_copy(src, dst, load_sem.at[i])
        for i, (src, dst) in enumerate([(pd_hbm, pd), (pl_hbm, plist), (sd_hbm, sd), (sl_hbm, sl), (sr_hbm, sr)])
    ]
    for copy in small:
        copy.start()
    whole = pltpu.make_async_copy(q_hbm, queries, load_sem.at[5])
    whole.start()
    counts = pltpu.make_async_copy(len_hbm, len_ref, load_sem.at[6])
    counts.start()
    pre_copies = [
        pltpu.make_async_copy(docs_hbm.at[:, :, columns(k)], pre_docs.at[k], docs_sem.at[k]) for k in range(head)
    ]
    top_copies = [
        pltpu.make_async_copy(docs_hbm.at[:, pl.ds(0, SHORT_ROWS), columns(k)], top_docs.at[k - head], docs_sem.at[k])
        for k in range(head, full // LANES)
    ]
    for copy in pre_copies + top_copies:
        copy.start()
    for copy in small:
        copy.wait()
    codes = jnp.concatenate([x[...].astype(jnp.float32) for x in (pd, plist, sd, sl, sr)], axis=1)
    for k in range(head, gathered[0].shape[0]):
        gathered[0][k, 0] = codes[:, (k - head) * LANES:(k - head + 1) * LANES].astype(jnp.bfloat16)
    for copy in firsts:
        copy.wait()
    pl.semaphore_wait(barrier, line + ranks // 2 - 1)
    plane = [r for r in range(2, ranks, 2)]

    def push(c, source, target, n, recv, device):
        pltpu.make_async_remote_copy(
            src_ref=gathered[c].at[:, pl.ds(source, n)], dst_ref=gathered[c].at[:, pl.ds(target, n)],
            send_sem=send_sem.at[c], recv_sem=recv, device_id=device, device_id_type=MESH,
        ).start()

    def finish(part, sem):
        pltpu.make_async_copy(part, part, sem).wait()

    def arrived(c, n, sem):
        finish(gathered[c].at[:, pl.ds(0, n)], sem)

    def begin(c):
        for k in range(1, line):
            push(c, 0, k, 1, line_recv.at[c], (gx, (gy + k) % line))
        for r in plane:
            push(c, 0, slot(r, 0), 1, plane_recv.at[c], (across[r], gy))

    def spread(c):
        arrived(c, line - 1, line_recv.at[c])
        for r in plane:
            push(c, 1, slot(r, 1), line - 1, plane_recv.at[c], (across[r], gy))

    def share(c):
        arrived(c, len(plane) * line, plane_recv.at[c])
        push(c, 0, count // 2, count // 2, core_recv.at[c], (across[1], gy))

    def shared(c):
        arrived(c, count // 2, core_recv.at[c])

    begin(0)
    whole.wait()
    values = queries[...].astype(jnp.float32)
    norm = row_norm(values)
    for c in range(1, chunks):
        for k in range(gathered[c].shape[0]):
            at = cuts[c] + k * LANES
            gathered[c][k, 0] = (values[:, at:at + LANES] / norm).astype(jnp.bfloat16)
    for c in range(1, chunks):
        begin(c)

    def rows_of(c, t, ks):
        slots = slice(t * per_tile, (t + 1) * per_tile)
        return jnp.concatenate([gathered[c][k, slots].reshape(TILE, LANES) for k in ks], axis=1)

    def pack_tops(t):
        lane = lax.broadcasted_iota(jnp.int32, (8, LANES), 1)
        for u in range(TILE // LANES):
            turned = jnp.transpose(result[:, u * LANES:(u + 1) * LANES])
            for i in range(per_lane):
                low = turned[i * query_rows:i * query_rows + 8]
                high = pltpu.roll(turned[i * query_rows + 8:(i + 1) * query_rows], 64, 1)
                pair = jnp.where(lane < 64, low, high)
                swapped = pltpu.roll(pltpu.roll(pair, 4, 0), TOPK, 1)
                message = jnp.where(lane % 64 < TOPK, pair, swapped)[:packed]
                s = t * per_tile + u * per_lane + i
                if s == 0:
                    got[0] = message
                else:
                    ret[s] = message

    def give(source, target, sems, some):
        for s, r, k in places[some.start * per_tile:some.stop * per_tile]:
            if s == 0:
                continue
            pltpu.make_async_remote_copy(
                src_ref=source(s), dst_ref=target.at[s], send_sem=sems.at[0], recv_sem=sems.at[1],
                device_id=(across[r], (gy + line - k) % line), device_id_type=MESH,
            ).start()

    def give_parts(some):
        lanes = slice(some.start * TILE, some.stop * TILE)
        first = some.start * TILE // LANES
        for kind in range(2):
            sums = jnp.sum(acc[kind, :, lanes], axis=0, keepdims=True)
            for g in range(len(some) * TILE // LANES):
                part_ret[first + g, kind:kind + 1, :] = sums[:, g * LANES:(g + 1) * LANES]
        if some.start == 0:
            part_got[0] = part_ret[0]
        give(lambda s: part_ret.at[s // per_lane], part_got, part_sem, some)

    def prefix(t):
        lanes = slice(t * TILE, (t + 1) * TILE)
        raw = rows_of(0, t, range(head)).astype(jnp.float32)
        unit[lanes, :] = (raw / row_norm(raw)).astype(jnp.bfloat16)
        turned = jnp.transpose(rows_of(0, t, range(head, gathered[0].shape[0])).astype(jnp.float32))
        p_dev, p_list = turned[:probes], turned[probes:2 * probes]
        base = 2 * probes
        s_dev, s_list, s_row = (turned[base + i * shorts:base + (i + 1) * shorts] for i in range(3))
        probed = jnp.sum(jnp.where(p_dev == me, p_list + 1.0, 0.0), axis=0, keepdims=True).astype(jnp.int32) - 1
        at = s_list * SHORT_ROWS + s_row + 1.0
        wanted = jnp.sum(jnp.where(s_dev == me, at, 0.0), axis=0, keepdims=True).astype(jnp.int32) - 1
        spots[0:1, lanes] = wanted
        chunk = 32

        order = [slice(r, r + chunk) for r in range(0, rows, chunk)]
        limits = [jnp.where(probed == l, len_ref[l], 0) for l in range(lists)]
        for part in (order[:len(order) // 2], order[len(order) // 2:]):
            docs = jnp.concatenate([
                jnp.concatenate([pre_docs[k, :, some].reshape(lists * chunk, LANES) for k in range(head)], axis=1)
                for some in part
            ], axis=0)
            scores = lax.dot_general(docs, unit[lanes, :], NT, preferred_element_type=jnp.float32)
            for i, some in enumerate(part):
                place = lax.broadcasted_iota(jnp.int32, (chunk, TILE), 0) + some.start
                value = jnp.full((chunk, TILE), -jnp.inf, jnp.float32)
                for l in range(lists):
                    at = (i * lists + l) * chunk
                    value = jnp.where(place < limits[l], scores[at:at + chunk], value)
                chosen[t, some, :] = value

    def tops(t):
        for u in range(TILE // LANES):
            spot = slice(u * LANES, (u + 1) * LANES)
            v = [chosen[t, 8 * i:8 * i + 8, spot] for i in range(rows // 8)]
            parts = [sort_desc(v[i:i + TOPK]) for i in range(0, len(v), TOPK)]
            v = functools.reduce(merge_top, parts)
            for shift in (4, 2, 1):
                v = merge_top(v, [pltpu.roll(x, shift, 0) for x in v])
            sub = lax.broadcasted_iota(jnp.int32, (8, LANES), 0)
            for a in range(TOPK // 8):
                one = v[8 * a]
                for s in range(1, 8):
                    one = jnp.where(sub == s, v[8 * a + s], one)
                result[8 * a:8 * a + 8, spot] = one
        pack_tops(t)

    def rescore(c, t):
        lanes = slice(t * TILE, (t + 1) * TILE)
        width = cuts[c + 1] - cuts[c]
        wanted = spots[0:1, lanes]
        place = lax.broadcasted_iota(jnp.int32, (SHORT_ROWS, TILE), 0)
        kind = 0 if c == 0 else 1
        ks = range(width // LANES)
        tall = [pre_docs[k, :, :SHORT_ROWS] if c == 0 else top_docs[cuts[c] // LANES - head + k] for k in ks]
        docs = jnp.concatenate([x.reshape(lists * SHORT_ROWS, LANES) for x in tall], axis=1)
        scores = lax.dot_general(docs, rows_of(c, t, ks), NT, preferred_element_type=jnp.float32)
        sums = jnp.zeros((8, TILE), jnp.float32) if c < 2 else acc[kind, :, lanes]
        for j in range(lists):
            hit = place == wanted - j * SHORT_ROWS
            part = jnp.where(hit, scores[j * SHORT_ROWS:(j + 1) * SHORT_ROWS], 0.0)
            sums = sums + jnp.sum(part.reshape(SHORT_ROWS // 8, 8, TILE), axis=0)
        acc[kind, :, lanes] = sums

    halves = (range(tiles // 2), range(tiles // 2, tiles))
    for c in range(chunks):
        spread(c)
    share(0)
    counts.wait()
    for copy in pre_copies:
        copy.wait()
    for t in halves[0]:
        prefix(t)
    shared(0)
    for t in halves[0]:
        tops(t)
    for t in halves[1]:
        prefix(t)
    share(1)
    for t in range(tiles):
        rescore(0, t)
    for t in halves[1]:
        tops(t)
    for copy in top_copies:
        copy.wait()
    for c in range(1, chunks):
        if c + 1 < chunks:
            share(c + 1)
        shared(c)
        for t in range(tiles):
            rescore(c, t)
        if c == chunks - 3:
            give(lambda s: ret.at[s], got, top_sem, range(tiles))
    give_parts(range(tiles))

    finish(got.at[pl.ds(0, count - 1)], top_sem.at[1])
    v = [jnp.concatenate([got[i], got[i + 1]], axis=0) for i in range(0, count, 2)]
    parts = [sort_desc(v[i:i + TOPK]) for i in range(0, len(v), TOPK)]
    best = functools.reduce(merge_top, parts)
    best = merge_top(best, [pltpu.roll(x, 4, 0) for x in best])
    shift = TOPK // 2
    while shift:
        best = merge_top(best, [pltpu.roll(x, LANES - shift, 1) for x in best])
        shift //= 2
    lane = lax.broadcasted_iota(jnp.int32, (8, LANES), 1)
    out = best[0]
    for i in range(1, TOPK):
        out = jnp.where(lane % TOPK == i, pltpu.roll(best[i], i, 1), out)
    for g in range(LANES // TOPK):
        moved = out if g == 0 else pltpu.roll(out, LANES - g * TOPK, 1)
        out_ref[g * packed:(g + 1) * packed, :TOPK] = moved[:packed, :TOPK]

    finish(part_got.at[pl.ds(0, count - 1)], part_sem.at[1])
    lane = lax.broadcasted_iota(jnp.int32, (count, LANES), 1)
    owner = lax.broadcasted_iota(jnp.int32, (count, LANES), 0) % per_lane
    sums = []
    for kind in range(2):
        kept = jnp.where(lane // query_rows == owner, part_got[:, kind, :], 0.0)
        sums.append(jnp.sum(jnp.transpose(kept).reshape(per_lane, query_rows, count), axis=0))
    rescored = sums[0] / norm + sums[1]
    dev = sd[...]
    picked = jnp.zeros((query_rows, shorts), jnp.float32)
    for s, r, k in places:
        there = across[r] * line + (gy + k) % line
        picked = jnp.where(dev == there, rescored[:, s:s + 1], picked)
    out_ref[:, TOPK:] = picked

    for c in range(chunks):
        arrived(c, count - 1, send_sem.at[c])
    finish(got.at[pl.ds(0, count - 1)], top_sem.at[0])
    finish(part_got.at[pl.ds(0, count - 1)], part_sem.at[0])


def shards(queries, probe_dev, probe_list, documents, lengths, short_dev, short_list, short_row):
    count = lax.axis_size(AXES)
    lists, rows, full = documents.shape
    query_rows = queries.shape[0]
    probes, shorts = probe_dev.shape[1], short_dev.shape[1]
    total = count * query_rows
    cuts = column_cuts(full)
    chunks = len(cuts) - 1
    packed = query_rows * TOPK // LANES
    extra = 2 * probes + 3 * shorts
    vmem = pl.BlockSpec(memory_space=pltpu.VMEM)
    hbm = pl.BlockSpec(memory_space=pltpu.HBM)
    dma = pltpu.SemaphoreType.DMA
    out = pl.pallas_call(
        search_kernel,
        out_shape=jax.ShapeDtypeStruct((query_rows, TOPK + shorts), jnp.float32),
        in_specs=[hbm] * 8,
        out_specs=vmem,
        scratch_shapes=[
            pltpu.VMEM(
                ((cuts[c + 1] - cuts[c] + (extra if c == 0 else 0)) // LANES, count, query_rows, LANES), jnp.bfloat16
            )
            for c in range(chunks)
        ] + [
            pltpu.VMEM((query_rows, full), jnp.bfloat16),
            pltpu.SMEM((lists,), jnp.int32),
            pltpu.VMEM((query_rows, probes), jnp.int32),
            pltpu.VMEM((query_rows, probes), jnp.int32),
            pltpu.VMEM((query_rows, shorts), jnp.int32),
            pltpu.VMEM((query_rows, shorts), jnp.int32),
            pltpu.VMEM((query_rows, shorts), jnp.int32),
            pltpu.VMEM((PREFIX // LANES, lists, rows, LANES), jnp.bfloat16),
            pltpu.VMEM(((full - PREFIX) // LANES, lists, SHORT_ROWS, LANES), jnp.bfloat16),
            pltpu.VMEM((total, PREFIX), jnp.bfloat16),
            pltpu.VMEM((8, total), jnp.int32),
            pltpu.VMEM((total // TILE, rows, TILE), jnp.float32),
            pltpu.VMEM((LANES, TILE), jnp.float32),
            pltpu.VMEM((count, packed, LANES), jnp.float32),
            pltpu.VMEM((count, packed, LANES), jnp.float32),
            pltpu.VMEM((2, 8, total), jnp.float32),
            pltpu.VMEM((total // LANES, 2, LANES), jnp.float32),
            pltpu.VMEM((count, 2, LANES), jnp.float32),
            dma((9,)),
            dma((full // LANES,)),
            dma((chunks,)),
            dma((chunks,)),
            dma((chunks,)),
            dma((chunks,)),
            dma((2,)),
            dma((2,)),
        ],
        compiler_params=pltpu.CompilerParams(
            collective_id=0, has_side_effects=True, vmem_limit_bytes=60 * 1024 * 1024
        ),
        name="search",
    )(queries, probe_dev, probe_list, short_dev, short_list, short_row, lengths, documents)
    return out[:, :TOPK], out[:, TOPK:]


def solution(mesh):
    one = P(AXES, None)
    in_specs = (one, one, one, P(AXES, None, None), P(AXES), one, one, one)
    return jax.shard_map(shards, mesh=mesh, in_specs=in_specs, out_specs=(one, one), check_vma=False)
```
